32 devices in a mesh: row: 8 (over z, x), col: 4 (over y, core).
Axes of the slice: x: 2, y: 2, z: 4, core: 2. Of those that a mesh axis runs over, the one named last changes fastest.
Arguments:
- gradients: bfloat16 [8, 4, 4, 64, 1536], P('row', 'col'), may hold values from -96 to 96
- token_counts: int32 [8, 4], P('row', 'col'), may hold values from 16 to 256
- row_groups: int32 [2, 8, 4], replicated, may hold values from 0 to 3, each once within a row
- col_groups: int32 [1, 4, 8], replicated, may hold values from 0 to 7, each once within a row
Outputs:
- averaged: float32 [8, 4, 4, 64, 1536], P('row', 'col')
- totals: int32 [8, 4], P('row', 'col')
The draws below stay inside these ranges and needn't reach their ends.
Inputs may be any that keep to these rules, and one draw needn't show every extreme that they name: row_groups[r, i] lists the 4 grid columns in some order: in row round r, grid row i's member of group g sits in column row_groups[r, i, g]. col_groups[0, j] lists the 8 grid rows in some order: grid column j's member of group h sits in row col_groups[0, j, h].
All inputs are finite; a program needn't handle non-finite values.
Results may differ from the reference program's by a relative error of at most 0.0003.
Values may be sent and summed in bfloat16 or wider, within the bound.
No kernel may reach another device: no remote copies, remote signals or barrier semaphores. Data moves between devices by JAX's collectives and lax.ppermute only.
A program may use at most 64 MiB of HBM per device.

```python
import jax
import jax.numpy as jnp

D = 1536
BLOCKS = 4
GR = 64
N_ROW = 8
N_COL = 4


def with_ends(drawn, rng, smallest, largest):
    spot = [jax.random.randint(jax.random.fold_in(rng, axis), (), 0, length) for axis, length in enumerate(drawn.shape)]
    widest = drawn.shape.index(max(drawn.shape))
    beside = spot[:widest] + [(spot[widest] + 1) % drawn.shape[widest]] + spot[widest + 1:]
    return drawn.at[tuple(spot)].set(smallest).at[tuple(beside)].set(largest)


def block_scale(rng, dims, split, smallest, high):
    def one(dim, blocks):
        steps = jax.random.uniform(jax.random.fold_in(jax.random.fold_in(rng, 6), dim), (blocks,), jnp.float32, smallest / len(split), high / len(split))
        return jnp.repeat(jnp.exp(steps), dims[dim] // blocks).reshape((-1,) + (1,) * (len(dims) - dim - 1))

    level = one(*split[0])
    for cut in split[1:]:
        level = level * one(*cut)
    return level


def centred(rng, extent, deviation, reach, pieces=(), dtype=jnp.bfloat16):
    array = deviation * jax.random.normal(rng, extent, jnp.float32)
    if pieces:
        array = array * block_scale(rng, extent, pieces, -0.22, 0.18)
    return jnp.clip(array, -reach, reach).astype(dtype)


def setup_inputs(seed: int = 0) -> dict:
    seeds = jax.random.split(jax.random.key(seed), 5)
    return {
        "gradients": centred(seeds[0], (N_ROW, N_COL, BLOCKS, GR, D), 16.0, 96.0, ((0, 8), (1, 4))),
        "token_counts": with_ends(jax.random.randint(seeds[1], (N_ROW, N_COL), 16, 257), jax.random.fold_in(seeds[1], 1), 16, 256).astype(jnp.int32),
        "row_groups": jax.vmap(lambda own: jax.random.permutation(own, N_COL))(jax.random.split(seeds[2], 2 * N_ROW)).reshape((2, N_ROW, N_COL)).astype(jnp.int32),
        "col_groups": jax.vmap(lambda own: jax.random.permutation(own, N_ROW))(jax.random.split(seeds[3], 1 * N_COL)).reshape((1, N_COL, N_ROW)).astype(jnp.int32),
    }


def groups_average(values, weights, group_order):
    picked = jnp.take_along_axis(values, group_order[:, :, None, None], axis=1)
    picked_w = jnp.take_along_axis(weights, group_order, axis=1)
    group_sums = jnp.sum(picked * picked_w[:, :, None, None], axis=0)
    group_totals = jnp.sum(picked_w, axis=0)
    averaged = group_sums / group_totals[:, None, None]
    inverse = jnp.argsort(group_order, axis=1).astype(jnp.int32)
    return averaged[inverse], group_totals[inverse]


def reference(gradients, token_counts, row_groups, col_groups):
    grad_state = gradients.reshape(N_ROW, N_COL, BLOCKS * GR, D).astype(jnp.float32)
    weight = token_counts.astype(jnp.float32)
    grad_state, weight = groups_average(grad_state, weight, row_groups[0])
    swapped, swapped_w = groups_average(jnp.swapaxes(grad_state, 0, 1), weight.T, col_groups[0])
    grad_state = jnp.swapaxes(swapped, 0, 1)
    weight = swapped_w.T
    grad_state, weight = groups_average(grad_state, weight, row_groups[1])
    return grad_state.reshape(gradients.shape), weight.astype(jnp.int32)
```

```python
import functools

import jax
import jax.numpy as jnp
from jax import lax
from jax.experimental import pallas as pl
from jax.experimental.pallas import tpu as pltpu
from jax.sharding import PartitionSpec as P

GRID = ("row", "col")
TOP = 60000.0
TAIL = 128
CUTS = 4
SMEM = pl.BlockSpec(memory_space=pltpu.SMEM)
VMEM = pl.BlockSpec(memory_space=pltpu.VMEM)
ROOM = pltpu.CompilerParams(vmem_limit_bytes=16 * 2**20)


def one_hot(values, count):
    return (values[..., None] == jnp.arange(count, dtype=jnp.int32)).astype(jnp.float32)


def path_counts(row_groups, col_groups):
    rows, cols = row_groups.shape[1:]
    first = one_hot(row_groups[0], cols)
    second = one_hot(col_groups[0], rows)
    third = one_hot(row_groups[1], cols)
    exact = functools.partial(jnp.einsum, precision=lax.Precision.HIGHEST)
    two = exact("jhi,igj->hg", second, first)
    three = exact("ikj,jhi->kh", third, second)
    paths = exact("kg,igj->kij", exact("kh,hg->kg", three, two), first)
    numbers = jnp.arange(cols, dtype=jnp.float32)[None, :, None]
    group_of = jnp.sum(third * numbers, axis=1).astype(jnp.int32)
    return paths.reshape(cols, rows * cols), group_of.reshape(-1)


def pack_kernel(count, gradients, out, sems):
    height, width = gradients.shape
    cut = height // CUTS
    copies = []
    for n in range(CUTS):
        part = pl.ds(n * cut, cut)
        copy = pltpu.make_async_copy(
            gradients.at[part, :], out.at[part, pl.ds(0, width)], sems.at[n]
        )
        copy.start()
        copies.append(copy)
    peak = jnp.zeros((1, width), jnp.float32)
    for n, copy in enumerate(copies):
        copy.wait()
        x = out[pl.ds(n * cut, cut), pl.ds(0, width)].astype(jnp.float32)
        peak = jnp.maximum(peak, jnp.max(jnp.abs(x), axis=0, keepdims=True))
    highest = jnp.max(peak, axis=1, keepdims=True)
    lane = lax.broadcasted_iota(jnp.int32, (height, TAIL), 1)
    tail = jnp.where(lane < TAIL // 2, count[0].astype(jnp.float32), highest)
    out[:, pl.ds(width, TAIL)] = tail.astype(out.dtype)


def mix_kernel(paths, pieces, coded, facts):
    groups, replicas = paths.shape
    step = 4 if replicas % 4 == 0 else 1
    width = pieces.shape[2] - TAIL
    height = pieces.shape[1]
    lanes = width // 2 if width % 256 == 0 else width
    for k0 in range(0, groups, 4):
        ks = range(k0, min(k0 + 4, groups))
        for c in range(0, width, lanes):

            def body(s, held):
                for u in range(step):
                    at = s * step + u
                    x = pieces[at, :, c:c + lanes].astype(jnp.float32)
                    tail = pieces[at, :, width:].astype(jnp.float32)
                    w, m = tail[:, :1], tail[:, TAIL - 1:]
                    sums, totals, bounds = held
                    shares = tuple(paths[k, at] * w for k in ks)
                    sums = tuple(a + q * x for a, q in zip(sums, shares))
                    totals = tuple(a + q for a, q in zip(totals, shares))
                    bounds = tuple(a + q * m for a, q in zip(bounds, shares))
                    held = (sums, totals, bounds)
                return held

            def zeros(wide):
                return tuple(jnp.zeros((height, wide), jnp.float32) for _ in ks)

            start = (zeros(lanes), zeros(1), zeros(1))
            sums, totals, bounds = lax.fori_loop(0, replicas // step, body, start)
            for a, t, b, k in zip(sums, totals, bounds, ks):
                unit = a * jnp.where(b > 0.0, 1.0 / b, 0.0)
                coded[k, :, c:c + lanes] = unit * jnp.abs(unit) * TOP
                lane = lax.broadcasted_iota(jnp.int32, (height, TAIL), 1)
                facts[k] = jnp.where(lane == 0, t, b / t)


def local(gradients, token_counts, row_groups, col_groups):
    rows, cols = lax.axis_size("row"), lax.axis_size("col")
    replicas = rows * cols
    place = lax.axis_index("row") * cols + lax.axis_index("col")
    width = gradients.shape[-1]
    flat = gradients.reshape(-1, width)
    packed = pl.pallas_call(
        pack_kernel,
        in_specs=[SMEM, pl.BlockSpec(memory_space=pl.ANY)],
        out_specs=VMEM,
        out_shape=jax.ShapeDtypeStruct((flat.shape[0], width + TAIL), flat.dtype),
        scratch_shapes=[pltpu.SemaphoreType.DMA((CUTS,))],
        compiler_params=ROOM,
    )(token_counts.reshape(1), flat)
    pieces = packed.reshape(replicas, -1, width + TAIL)
    arrived = lax.all_to_all(pieces, GRID, split_axis=0, concat_axis=0, tiled=True)
    height = arrived.shape[1]
    paths, group_of = path_counts(row_groups, col_groups)
    coded, facts = pl.pallas_call(
        mix_kernel,
        in_specs=[SMEM, VMEM],
        out_specs=(VMEM, VMEM),
        out_shape=(
            jax.ShapeDtypeStruct((cols, height, width), jnp.float32),
            jax.ShapeDtypeStruct((cols, height, TAIL), jnp.float32),
        ),
        compiler_params=ROOM,
    )(paths, arrived)
    chosen = coded[0][None]
    for k in range(1, cols):
        chosen = jnp.where((group_of == k)[:, None, None], coded[k][None], chosen)
    chosen = chosen.astype(jnp.float16)
    returned = lax.all_to_all(chosen, GRID, split_axis=0, concat_axis=0, tiled=True)
    own = (jnp.arange(cols) == group_of[place])[:, None]
    total, bound = jnp.sum(jnp.where(own, facts[:, 0, :2], 0.0), axis=0)
    code = returned.astype(jnp.float32)
    root = lax.rsqrt(jnp.maximum(jnp.abs(code), 1e-12))
    averaged = code * root * (bound * TOP ** -0.5)
    return (
        averaged.reshape(gradients.shape),
        total.astype(jnp.int32).reshape(token_counts.shape),
    )


def solution(mesh):
    placed = (P(*GRID, None, None, None), P(*GRID), P(), P())
    return jax.shard_map(
        local,
        mesh=mesh,
        in_specs=placed,
        out_specs=(P(*GRID, None, None, None), P(*GRID)),
        check_vma=False,
    )
```

```python
import functools

import jax
import jax.numpy as jnp
from jax import lax
from jax.experimental import pallas as pl
from jax.experimental.pallas import tpu as pltpu
from jax.sharding import PartitionSpec as P

GRID = ("row", "col")
TOP = 60000.0
TAIL = 128
CUTS = 8
SMEM = pl.BlockSpec(memory_space=pltpu.SMEM)
VMEM = pl.BlockSpec(memory_space=pltpu.VMEM)
HBM = pl.BlockSpec(memory_space=pltpu.HBM)
ROOM = pltpu.CompilerParams(vmem_limit_bytes=16 * 2**20)


def one_hot(values, count):
    return (values[..., None] == jnp.arange(count, dtype=jnp.int32)).astype(jnp.float32)


def path_counts(row_groups, col_groups):
    rows, cols = row_groups.shape[1:]
    first = one_hot(row_groups[0], cols)
    second = one_hot(col_groups[0], rows)
    third = one_hot(row_groups[1], cols)
    exact = functools.partial(jnp.einsum, precision=lax.Precision.HIGHEST)
    two = exact("jhi,igj->hg", second, first)
    three = exact("ikj,jhi->kh", third, second)
    paths = exact("kg,igj->kij", exact("kh,hg->kg", three, two), first)
    numbers = jnp.arange(cols, dtype=jnp.float32)[None, :, None]
    group_of = jnp.sum(third * numbers, axis=1).astype(jnp.int32)
    return paths.reshape(cols, rows * cols), group_of.reshape(-1)


def pack_kernel(token, gradients, out, held, tail, count, sems):
    height, width = gradients.shape
    cut = height // CUTS
    fetch = pltpu.make_async_copy(token, count, sems.at[2 * CUTS])
    fetch.start()
    arriving, leaving = [], []
    for n in range(CUTS):
        part = pl.ds(n * cut, cut)
        copy = pltpu.make_async_copy(gradients.at[part, :], held.at[part, :], sems.at[n])
        copy.start()
        arriving.append(copy)
    peak = jnp.zeros((1, width), jnp.float32)
    for n, copy in enumerate(arriving):
        part = pl.ds(n * cut, cut)
        copy.wait()
        copy = pltpu.make_async_copy(
            held.at[part, :], out.at[part, pl.ds(0, width)], sems.at[CUTS + n]
        )
        copy.start()
        leaving.append(copy)
        x = held[part, :].astype(jnp.float32)
        peak = jnp.maximum(peak, jnp.max(jnp.abs(x), axis=0, keepdims=True))
    highest = jnp.max(peak, axis=1, keepdims=True)
    fetch.wait()
    lane = lax.broadcasted_iota(jnp.int32, (height, TAIL), 1)
    facts = jnp.where(lane < TAIL // 2, count[0, 0].astype(jnp.float32), highest)
    tail[...] = facts.astype(tail.dtype)
    copy = pltpu.make_async_copy(tail, out.at[:, pl.ds(width, TAIL)], sems.at[2 * CUTS + 1])
    copy.start()
    leaving.append(copy)
    for copy in leaving:
        copy.wait()


def mix_kernel(paths, pieces, coded, facts, counts):
    groups, replicas = paths.shape
    step = 4 if replicas % 4 == 0 else 1
    stride = 32 if replicas % 32 == 0 else step
    width = pieces.shape[2] - TAIL
    height = pieces.shape[1]
    lanes = width // 2 if width % 256 == 0 else TAIL
    shape = (height, TAIL)

    def zeros(number):
        return tuple(jnp.zeros(shape, jnp.float32) for _ in range(number))

    for k0 in range(0, groups, 4):
        ks = range(k0, min(k0 + 4, groups))

        def head(s, held):
            for u in range(stride):
                at = s * stride + u
                tail = pieces[at, :, width:].astype(jnp.float32)
                w = jnp.broadcast_to(tail[:, :1], shape)
                wm = w * jnp.broadcast_to(tail[:, TAIL - 1:], shape)
                counts[at] = w
                totals, bounds = held
                totals = tuple(a + paths[k, at] * w for a, k in zip(totals, ks))
                bounds = tuple(a + paths[k, at] * wm for a, k in zip(bounds, ks))
                held = (totals, bounds)
            return held

        start = (zeros(len(ks)), zeros(len(ks)))
        totals, bounds = lax.fori_loop(0, replicas // stride, head, start)
        lane = lax.broadcasted_iota(jnp.int32, shape, 1)
        inverse = []
        for t, b, k in zip(totals, bounds, ks):
            facts[k] = jnp.where(lane == 0, t, b / t)
            inverse.append(jnp.where(b > 0.0, 1.0 / b, 0.0))
        for c in range(0, width, lanes):
            columns = range(c, c + lanes, TAIL)

            def body(s, sums):
                for u in range(step):
                    at = s * step + u
                    w = counts[at]
                    shares = tuple(paths[k, at] * w for k in ks)
                    xs = tuple(pieces[at, :, l:l + TAIL].astype(jnp.float32) for l in columns)
                    sums = tuple(
                        tuple(a + q * x for a, x in zip(line, xs)) for line, q in zip(sums, shares)
                    )
                return sums

            start = tuple(zeros(len(columns)) for _ in ks)
            sums = lax.fori_loop(0, replicas // step, body, start)
            for line, i, k in zip(sums, inverse, ks):
                for a, l in zip(line, columns):
                    unit = a * i
                    coded[k, :, l:l + TAIL] = unit * jnp.abs(unit) * TOP


def local(gradients, token_counts, row_groups, col_groups):
    rows, cols = lax.axis_size("row"), lax.axis_size("col")
    replicas = rows * cols
    place = lax.axis_index("row") * cols + lax.axis_index("col")
    width = gradients.shape[-1]
    flat = gradients.reshape(-1, width)
    packed = pl.pallas_call(
        pack_kernel,
        in_specs=[HBM, HBM],
        out_specs=HBM,
        out_shape=jax.ShapeDtypeStruct((flat.shape[0], width + TAIL), flat.dtype),
        scratch_shapes=[
            pltpu.VMEM(flat.shape, flat.dtype),
            pltpu.VMEM((flat.shape[0], TAIL), flat.dtype),
            pltpu.SMEM((1, 1), jnp.int32),
            pltpu.SemaphoreType.DMA((2 * CUTS + 2,)),
        ],
    )(token_counts, flat)
    pieces = packed.reshape(replicas, -1, width + TAIL)
    arrived = lax.all_to_all(pieces, GRID, split_axis=0, concat_axis=0, tiled=True)
    height = arrived.shape[1]
    paths, group_of = path_counts(row_groups, col_groups)
    coded, facts = pl.pallas_call(
        mix_kernel,
        in_specs=[SMEM, VMEM],
        out_specs=(VMEM, VMEM),
        out_shape=(
            jax.ShapeDtypeStruct((cols, height, width), jnp.float32),
            jax.ShapeDtypeStruct((cols, height, TAIL), jnp.float32),
        ),
        scratch_shapes=[pltpu.VMEM((replicas, height, TAIL), jnp.float32)],
        compiler_params=ROOM,
    )(paths, arrived)
    chosen = coded[0][None]
    for k in range(1, cols):
        chosen = jnp.where((group_of == k)[:, None, None], coded[k][None], chosen)
    chosen = chosen.astype(jnp.float16)
    returned = lax.all_to_all(chosen, GRID, split_axis=0, concat_axis=0, tiled=True)
    own = (jnp.arange(cols) == group_of[place])[:, None]
    total, bound = jnp.sum(jnp.where(own, facts[:, 0, :2], 0.0), axis=0)
    code = returned.astype(jnp.float32)
    root = lax.rsqrt(jnp.maximum(jnp.abs(code), 1e-12))
    averaged = code * root * (bound * TOP ** -0.5)
    return (
        averaged.reshape(gradients.shape),
        total.astype(jnp.int32).reshape(token_counts.shape),
    )


def solution(mesh):
    placed = (P(*GRID, None, None, None), P(*GRID), P(), P())
    return jax.shard_map(
        local,
        mesh=mesh,
        in_specs=placed,
        out_specs=(P(*GRID, None, None, None), P(*GRID)),
        check_vma=False,
    )
```
